32 devices in a mesh: clips: 2 (over x), tm: 4 (over y, core), height: 4 (over z).
Axes of the slice: x: 2, y: 2, z: 4, core: 2. Of those that a mesh axis runs over, the one named last changes fastest.
Arguments:
- features: bfloat16 [16, 16, 96, 512], P(('clips', 'tm'), 'height'), parts along dimension 0, may hold values from -1000 to 1000
- gain: float32 [512], replicated, may hold values from 0.1 to 1.9
- shift: float32 [512], replicated, may hold values from -3 to 3
- kernel: bfloat16 [3, 3, 3, 512, 256], replicated, may hold values from -0.0546875 to 0.0546875
- bias: float32 [256], replicated, may hold values from -3 to 3
Outputs:
- decoded: bfloat16 [16, 16, 96, 256], P(('clips', 'tm'), 'height'), parts along dimension 0
The draws below stay inside these ranges and needn't reach their ends.
There are 2 independent parts, one for each index of `clips`. The reference program is written for one: setup_inputs(seed, part) draws one part's arguments, and reference() takes and returns one part's arrays. A program takes and returns all parts, laid end to end along the dimension named above; an argument that names none is the same for every part. Nothing has to cross between parts.
All inputs are finite; a program needn't handle non-finite values.
Results may differ from the reference program's by a relative error of at most 0.0055.
Values may be sent and summed in bfloat16 or wider, within the bound.
A program may use at most 64 MiB of HBM per device.

```python
import jax
import jax.numpy as jnp
from jax import lax

CHANNELS = 512
COUT = 256
GROUPS = 32
COLS = 96
FRAMES = 8
ROWS = 16


def draw_features(key, part):
    keys = jax.random.split(jax.random.fold_in(key, 17), 5)
    frame_pos = jnp.arange(FRAMES, dtype=jnp.float32) / max(FRAMES - 1, 1)
    frame_trend = jnp.exp(jnp.log(3.0) * frame_pos)
    chan_scale = jnp.exp(jax.random.uniform(keys[1], (CHANNELS,), jnp.float32, 0.0, jnp.log(10.0)))
    chan_offset = 0.5 * jax.random.normal(keys[2], (CHANNELS,), jnp.float32)
    noise = jnp.clip(jax.random.normal(keys[0], (FRAMES, ROWS, COLS, CHANNELS), jnp.float32), -6.0, 6.0)
    frame_random = jnp.exp(jax.random.uniform(keys[4], (FRAMES,), jnp.float32, -jnp.log(2.0), jnp.log(2.0)))
    frame_scale = frame_trend * frame_random
    values = (noise + chan_offset) * chan_scale
    values = values * frame_scale[:, None, None, None]
    values = jnp.clip(values, -1000.0, 1000.0)
    return values.astype(jnp.bfloat16)


def bell_draw(stream_key, extent, deviation, reach, held_as=jnp.bfloat16):
    result = deviation * jax.random.normal(stream_key, extent, jnp.float32)
    return jnp.clip(result, min=-reach, max=reach).astype(held_as)


def setup_inputs(seed: int = 0, part: int = 0) -> dict:
    key_list = jax.random.split(jax.random.key(seed), 6)
    part_splits = jax.random.split(jax.random.fold_in(key_list[5], part), 6)
    features = draw_features(jax.random.fold_in(jax.random.fold_in(key_list[5], part), 71), part)
    gain = jnp.clip(1.0 + 0.18 * jax.random.normal(key_list[1], (CHANNELS,), jnp.float32), 0.1, 1.9)
    shift = bell_draw(key_list[2], (CHANNELS,), 0.5, 3.0, jnp.float32)
    kernel = bell_draw(key_list[3], (3, 3, 3, CHANNELS, COUT), (27 * CHANNELS) ** -0.5, 0.0546875)
    bias = bell_draw(key_list[4], (COUT,), 0.5, 3.0, jnp.float32)
    return {"features": features, "gain": gain, "shift": shift, "kernel": kernel, "bias": bias}


epsilon = 1e-06

def reference(features, gain, shift, kernel, bias):
    per_group = CHANNELS // GROUPS
    wide_values = features.astype(jnp.float32).reshape(FRAMES, ROWS, COLS, GROUPS, per_group)
    cells_total = FRAMES * ROWS * COLS * per_group
    group_mean = lax.optimization_barrier(jnp.sum(wide_values, axis=(0, 1, 2, 4))) / cells_total
    centered = wide_values - group_mean[:, None]
    group_var = lax.optimization_barrier(jnp.sum(centered * centered, axis=(0, 1, 2, 4))) / cells_total
    normed = centered * lax.rsqrt(group_var + epsilon)[:, None]
    normed = normed.reshape(FRAMES, ROWS, COLS, CHANNELS) * gain + shift
    activated = jax.nn.silu(normed).astype(jnp.bfloat16)
    padded = jnp.concatenate([activated[:1], activated[:1], activated], 0)
    padded = jnp.pad(padded, ((0, 0), (1, 1), (1, 1), (0, 0)))

    def one_frame(position):
        slab = lax.dynamic_slice_in_dim(padded, position, 3, 0)
        summed = jnp.zeros((ROWS * COLS, COUT), jnp.float32)
        for a in range(3):
            for b in range(3):
                for c in range(3):
                    window = slab[a, b:b + ROWS, c:c + COLS, :].reshape(ROWS * COLS, CHANNELS)
                    summed = summed + jnp.dot(window, kernel[a, b, c], preferred_element_type=jnp.float32)
        return (summed.reshape(ROWS, COLS, COUT) + bias).astype(jnp.bfloat16)
    return lax.map(one_frame, jnp.arange(FRAMES, dtype=jnp.int32))
```

```python
import functools

import jax
import jax.numpy as jnp
from jax import lax
from jax.experimental import pallas as pl
from jax.experimental.pallas import tpu as pltpu
from jax.sharding import PartitionSpec as P

GROUPS = 32
EPSILON = 1e-06
MESH = pl.DeviceIdType.MESH
F32 = jnp.float32
BF16 = jnp.bfloat16


LANES = 128


def group_sums(values, group):
    lanes = values.shape[-1]
    lane = lax.broadcasted_iota(jnp.int32, values.shape, values.ndim - 1)
    step = 1
    while step < group:
        up = pltpu.roll(values, lanes - step, values.ndim - 1)
        down = pltpu.roll(values, step, values.ndim - 1)
        values = values + jnp.where((lane & step) == 0, up, down)
        step *= 2
    return values


def own_lanes(parts):
    lane = lax.broadcasted_iota(jnp.int32, (parts, LANES), 1)
    row = lax.broadcasted_iota(jnp.int32, (parts, LANES), 0)
    return lax.rem(lane, parts) == row


def body(
    n_tm,
    n_h,
    x_hbm,
    gain_hbm,
    shift_hbm,
    w_hbm,
    bias_hbm,
    out_ref,
    x_vm,
    small,
    w_vm,
    u_vm,
    top_vm,
    bot_vm,
    stats,
    lhs,
    prod,
    nbuf,
    rbuf,
    x_sem,
    p_sem,
    w_sem,
    s_send,
    s_recv,
    h_send,
    h_recv,
    n_send,
    n_recv,
):
    frames, rows, cols, channels = x_vm.shape
    c_out = w_vm.shape[-1]
    per_group = channels // GROUPS
    tm = lax.axis_index("tm")
    hh = lax.axis_index("height")

    barrier = pltpu.get_barrier_semaphore()
    count = n_tm * n_h
    me = tm * n_h + hh

    def peer(d):
        other = lax.rem(me + d, count)
        return {"tm": lax.div(other, n_h), "height": lax.rem(other, n_h)}

    for d in range(1, count):
        pl.semaphore_signal(barrier, inc=1, device_id=peer(d), device_id_type=MESH)
    half = rows // 2
    x_copies = [
        pltpu.make_async_copy(
            x_hbm.at[f, q * half : (q + 1) * half], x_vm.at[f, q * half : (q + 1) * half], x_sem.at[f, q]
        )
        for f in range(frames)
        for q in range(2)
    ]
    for copy in x_copies:
        copy.start()
    ends = (0, channels, 2 * channels, 2 * channels + c_out)
    for i, ref in enumerate((gain_hbm, shift_hbm, bias_hbm)):
        pltpu.make_async_copy(ref, small.at[:, ends[i] : ends[i + 1]], p_sem).start()
    w_copies = [
        pltpu.make_async_copy(w_hbm.at[:, :, c], w_vm.at[:, c], w_sem.at[c]) for c in range(3)
    ]
    with jax.named_scope("a_sums"):
        sums = jnp.zeros((8, channels), F32)
        squares = jnp.zeros((8, channels), F32)
        for p in range(2 * frames):
            with jax.named_scope("x_wait"):
                x_copies[p].wait()
            if p == 2 * frames - 1:
                for copy in w_copies:
                    copy.start()
            f = p // 2
            for r in range(p % 2 * half, p % 2 * half + half):
                v = x_vm[f, r].astype(F32).reshape(cols // 8, 8, channels)
                sums = sums + jnp.sum(v, axis=0)
                squares = squares + jnp.sum(v * v, axis=0)
    with jax.named_scope("b_stat"):
        blocks = channels // LANES
        parts = 2 * blocks
        assert parts <= per_group <= LANES
        sums = jnp.sum(sums, axis=0, keepdims=True)
        squares = jnp.sum(squares, axis=0, keepdims=True)
        stacked = jnp.concatenate(
            [v[:, k * LANES : (k + 1) * LANES] for v in (sums, squares) for k in range(blocks)], axis=0
        )
        spread = jnp.where(own_lanes(parts), group_sums(stacked, per_group), 0.0)
        stats[0] = jnp.sum(spread, axis=0, keepdims=True)

    with jax.named_scope("c_barrier"):
        pl.semaphore_wait(barrier, count - 1)

    shares = [
        pltpu.make_async_remote_copy(
            src_ref=stats.at[0],
            dst_ref=stats.at[d],
            send_sem=s_send,
            recv_sem=s_recv,
            device_id=peer(d),
            device_id_type=MESH,
        )
        for d in range(1, count)
    ]
    for copy in shares:
        copy.start()
    to_next = pltpu.make_async_remote_copy(
        src_ref=x_vm.at[:, rows - 1],
        dst_ref=top_vm,
        send_sem=h_send.at[0],
        recv_sem=h_recv.at[0],
        device_id={"height": lax.rem(hh + 1, n_h)},
        device_id_type=MESH,
    )
    to_last = pltpu.make_async_remote_copy(
        src_ref=x_vm.at[:, 0],
        dst_ref=bot_vm,
        send_sem=h_send.at[1],
        recv_sem=h_recv.at[1],
        device_id={"height": lax.rem(hh + n_h - 1, n_h)},
        device_id_type=MESH,
    )

    @pl.when(hh < n_h - 1)
    def _():
        to_next.start()

    @pl.when(hh > 0)
    def _():
        to_last.start()

    step = 64
    for c in range(3):
        with jax.named_scope("w_wait"):
            w_copies[c].wait()

        with jax.named_scope("w_trans"):
            for b in range(3):

                @pl.loop(0, channels // step)
                def _(i):
                    part = pl.ds(pl.multiple_of(i * step, step), step)
                    g0, g1, g2 = (w_vm[a, c, b, part].astype(F32) for a in range(3))
                    even = 0.5 * (g0 + g2)
                    odd = 0.5 * g1
                    u_vm[0, c, b, part] = (even + odd).astype(BF16)
                    u_vm[1, c, b, part] = (even - odd).astype(BF16)

    pltpu.make_async_copy(small, small, p_sem).wait()
    with jax.named_scope("e_shares"):
        pltpu.make_async_copy(stats.at[1:], stats.at[1:], s_recv).wait()
    total = jnp.sum(stats[...], axis=0)
    cells = n_tm * n_h * frames * rows * cols * per_group
    means = group_sums(jnp.where(own_lanes(parts), total, 0.0), parts) * (1.0 / cells)
    mean = means[:blocks]
    var = jnp.maximum(means[blocks:] - mean * mean, 0.0)
    inverse = lax.rsqrt(var + EPSILON)

    def one_row(v):
        return jnp.concatenate([v[k : k + 1] for k in range(blocks)], axis=1)

    half_scale = 0.5 * small[:, ends[0] : ends[1]] * one_row(inverse)
    half_offset = 0.5 * small[:, ends[1] : ends[2]] - one_row(mean) * half_scale

    def activate(v):
        h = v.astype(F32) * half_scale + half_offset
        return (h + h * jnp.tanh(h)).astype(BF16)

    first = jnp.where(tm == 0, 1.0, 0.0).astype(F32)
    at = [(u - first).astype(BF16) for u in (0.0, 1.0, -1.0)]

    def place(row, v0, v1):
        f0, f1 = activate(v0), activate(v1)
        for u in range(3):
            lhs[u, row + 1] = f0 + at[u] * f1
        lhs[3, row + 1] = f1

    with jax.named_scope("f_act"):
        for r in range(rows):
            place(r, x_vm[0, r], x_vm[1, r])

    m = 2 * cols
    position = lax.rem(lax.broadcasted_iota(jnp.int32, (m, 1), 0), cols)
    not_first = position != 0
    not_last = position != cols - 1
    row_sets = (tuple(range(1, rows - 1)), (0, rows - 1))

    def weights(u, c):
        ref = (w_vm.at[2], u_vm.at[0], u_vm.at[1], w_vm.at[0])[u]
        return ref[c].reshape(3 * channels, c_out)

    def product(u, s):
        def tap(c, depth=slice(None), r=slice(None)):
            rows_of = [
                jnp.concatenate([lhs[u, i + b] for i in row_sets[s][r]], axis=0) for b in range(3)
            ]
            return jnp.dot(
                jnp.concatenate(rows_of, axis=1)[:, depth],
                weights(u, c)[depth],
                preferred_element_type=F32,
            )

        def low_of(v):
            return jnp.where(not_first, pltpu.roll(v, 1, 0), 0.0)

        high = jnp.where(not_last, pltpu.roll(tap(2), m - 1, 0), 0.0)
        cut = 3 * channels // 2
        if u in (2, 3):
            low = low_of(tap(0, slice(0, cut))) + low_of(tap(0, slice(cut, None)))
        else:
            low = low_of(tap(0))
        prod[u, s] = low + high + tap(1)

    def sends(s, k):
        return pltpu.make_async_remote_copy(
            src_ref=nbuf.at[s, k],
            dst_ref=rbuf.at[s, k],
            send_sem=n_send,
            recv_sem=n_recv.at[s],
            device_id={"tm": lax.rem(tm + 1, n_tm)},
            device_id_type=MESH,
        )

    def send(s, k):
        @pl.when(tm < n_tm - 1)
        def _():
            sends(s, k).start()

    def early(s):
        product(3, s)
        nbuf[s, 1] = prod[3, s].astype(BF16)
        send(s, 1)
        product(0, s)
        product(1, s)
        product(2, s)
        later = prod[1, s] + prod[2, s] - prod[0, s] + first * prod[3, s]
        nbuf[s, 0] = later.astype(BF16)
        send(s, 0)

    with jax.named_scope("g_early0"):
        early(0)

    with jax.named_scope("h_halo"):
        @pl.when(hh > 0)
        def _():
            to_next.wait_recv()
            place(-1, top_vm[0], top_vm[1])

        @pl.when(hh == 0)
        def _():
            for u in range(4):
                lhs[u, 0] = jnp.zeros((cols, channels), BF16)

        @pl.when(hh < n_h - 1)
        def _():
            to_last.wait_recv()
            place(rows, bot_vm[0], bot_vm[1])

        @pl.when(hh == n_h - 1)
        def _():
            for u in range(4):
                lhs[u, rows + 1] = jnp.zeros((cols, channels), BF16)

    with jax.named_scope("i_early1"):
        early(1)

    bias = small[:, ends[2] : ends[3]]
    with jax.named_scope("k_out"):
        for s in range(2):

            @pl.when(tm > 0)
            def _():
                pltpu.make_async_copy(rbuf.at[s], rbuf.at[s], n_recv.at[s]).wait()

            for k in (1, 0):
                at_0, at_1, at_minus, at_inf = (prod[u, s] for u in range(4))
                if k == 1:
                    own = jnp.where(tm == 0, 2.0 * at_1 - at_0, at_1 - at_minus - at_inf)
                else:
                    own = jnp.where(tm == 0, 2.0 * at_1, at_0)
                earlier = jnp.where(tm == 0, 0.0, rbuf[s, k].astype(F32))
                value = (own + earlier + bias).astype(BF16)
                for q, i in enumerate(row_sets[s]):
                    out_ref[k, i] = value[q * cols : (q + 1) * cols]

    with jax.named_scope("l_tail"):
        pltpu.make_async_copy(stats.at[1:], stats.at[1:], s_send).wait()

        @pl.when(hh < n_h - 1)
        def _():
            to_next.wait_send()

        @pl.when(hh > 0)
        def _():
            to_last.wait_send()

        @pl.when(tm < n_tm - 1)
        def _():
            pltpu.make_async_copy(nbuf, nbuf, n_send).wait()


def solution(mesh):
    n_tm, n_h = mesh.shape["tm"], mesh.shape["height"]

    def on_device(features, gain, shift, kernel, bias):
        frames, rows, cols, channels = features.shape
        c_out = kernel.shape[-1]
        assert frames == 2 and rows == 4
        per_set = 2 * cols
        vmem = pl.BlockSpec(memory_space=pltpu.VMEM)
        hbm = pl.BlockSpec(memory_space=pltpu.HBM)
        dma = pltpu.SemaphoreType.DMA
        return pl.pallas_call(
            functools.partial(body, n_tm, n_h),
            out_shape=pltpu.VMEM((frames, rows, cols, c_out), BF16),
            in_specs=[hbm] * 5,
            out_specs=vmem,
            scratch_shapes=[
                pltpu.VMEM((frames, rows, cols, channels), BF16),
                pltpu.VMEM((1, 2 * channels + c_out), F32),
                pltpu.VMEM((3, 3, 3, channels, c_out), BF16),
                pltpu.VMEM((2, 3, 3, channels, c_out), BF16),
                pltpu.VMEM((frames, cols, channels), BF16),
                pltpu.VMEM((frames, cols, channels), BF16),
                pltpu.VMEM((n_tm * n_h, 1, LANES), F32),
                pltpu.VMEM((4, rows + 2, cols, channels), BF16),
                pltpu.VMEM((4, 2, per_set, c_out), F32),
                pltpu.VMEM((2, 2, per_set, c_out), BF16),
                pltpu.VMEM((2, 2, per_set, c_out), BF16),
                dma((frames, 2)),
                dma,
                dma((3,)),
                dma,
                dma,
                dma((2,)),
                dma((2,)),
                dma,
                dma((2,)),
            ],
            compiler_params=pltpu.CompilerParams(
                collective_id=0, has_side_effects=True, vmem_limit_bytes=67_043_328 - 640 * 2**10
            ),
        )(features, gain.reshape(1, -1), shift.reshape(1, -1), kernel, bias.reshape(1, -1))

    placed = (P(("clips", "tm"), "height", None, None), P(), P(), P(), P())
    return jax.shard_map(
        on_device,
        mesh=mesh,
        in_specs=placed,
        out_specs=P(("clips", "tm"), "height", None, None),
        check_vma=False,
    )
```

```python
import functools

import jax
import jax.numpy as jnp
from jax import lax
from jax.experimental import pallas as pl
from jax.experimental.pallas import tpu as pltpu
from jax.sharding import PartitionSpec as P

GROUPS = 32
EPSILON = 1e-06
MESH = pl.DeviceIdType.MESH
F32 = jnp.float32
BF16 = jnp.bfloat16


LANES = 128


def group_sums(values, group):
    lane = lax.rem(lax.broadcasted_iota(jnp.int32, values.shape, 1), group)
    terms = [values]
    for j in range(1, group):
        up = pltpu.roll(values, LANES - j, 1)
        down = pltpu.roll(values, group - j, 1)
        terms.append(jnp.where(lane < group - j, up, down))
    while len(terms) > 1:
        terms = [sum(terms[i : i + 2][1:], terms[i]) for i in range(0, len(terms), 2)]
    return terms[0]


def own_lanes(parts):
    lane = lax.broadcasted_iota(jnp.int32, (parts, LANES), 1)
    row = lax.broadcasted_iota(jnp.int32, (parts, LANES), 0)
    return lax.rem(lane, parts) == row


def body(
    n_tm,
    n_h,
    x_hbm,
    gain_hbm,
    shift_hbm,
    w_hbm,
    bias_hbm,
    out_ref,
    x_vm,
    small,
    w_vm,
    u_vm,
    top_vm,
    bot_vm,
    stats,
    lhs,
    prod,
    own,
    nbuf,
    rbuf,
    x_sem,
    p_sem,
    w_sem,
    s_send,
    s_recv,
    h_send,
    h_recv,
    n_send,
    n_recv,
):
    frames, rows, cols, channels = x_vm.shape
    c_out = w_vm.shape[-1]
    per_group = channels // GROUPS
    tm = lax.axis_index("tm")
    hh = lax.axis_index("height")

    barrier = pltpu.get_barrier_semaphore()
    count = n_tm * n_h
    me = tm * n_h + hh

    def peer(d):
        other = lax.rem(me + d, count)
        return {"tm": lax.div(other, n_h), "height": lax.rem(other, n_h)}

    half = rows // 2
    x_copies = [
        pltpu.make_async_copy(
            x_hbm.at[f, q * half : (q + 1) * half], x_vm.at[f, q * half : (q + 1) * half], x_sem.at[f, q]
        )
        for f in range(frames)
        for q in range(2)
    ]
    for copy in x_copies:
        copy.start()
    for d in range(1, count):
        pl.semaphore_signal(barrier, inc=1, device_id=peer(d), device_id_type=MESH)
    ends = (0, channels, 2 * channels, 2 * channels + c_out)
    for i, ref in enumerate((gain_hbm, shift_hbm, bias_hbm)):
        pltpu.make_async_copy(ref, small.at[:, ends[i] : ends[i + 1]], p_sem).start()
    w_copies = [
        pltpu.make_async_copy(w_hbm.at[:, :, c], w_vm.at[:, c], w_sem.at[c]) for c in range(3)
    ]
    with jax.named_scope("a_sums"):
        sums = jnp.zeros((8, channels), F32)
        squares = jnp.zeros((8, channels), F32)
        for p in range(2 * frames):
            with jax.named_scope("x_wait"):
                x_copies[p].wait()
            if p == 2 * frames - 1:
                for copy in w_copies:
                    copy.start()
            f = p // 2
            for r in range(p % 2 * half, p % 2 * half + half):
                v = x_vm[f, r].astype(F32).reshape(cols // 8, 8, channels)
                sums = sums + jnp.sum(v, axis=0)
                squares = squares + jnp.sum(v * v, axis=0)
    with jax.named_scope("b_stat"):
        blocks = channels // LANES
        parts = 2 * blocks
        assert parts <= per_group <= LANES
        sums = jnp.sum(sums, axis=0, keepdims=True)
        squares = jnp.sum(squares, axis=0, keepdims=True)
        stacked = jnp.concatenate(
            [v[:, k * LANES : (k + 1) * LANES] for v in (sums, squares) for k in range(blocks)], axis=0
        )
        spread = jnp.where(own_lanes(parts), group_sums(stacked, per_group), 0.0)
        stats[0] = jnp.sum(spread, axis=0, keepdims=True)

    with jax.named_scope("c_barrier"):
        pl.semaphore_wait(barrier, count - 1)

    shares = [
        pltpu.make_async_remote_copy(
            src_ref=stats.at[0],
            dst_ref=stats.at[d],
            send_sem=s_send,
            recv_sem=s_recv,
            device_id=peer(d),
            device_id_type=MESH,
        )
        for d in range(1, count)
    ]
    for dh in (*range(1, n_h), 0):
        for dt in range(n_tm):
            if (dt, dh) != (0, 0):
                shares[dt * n_h + dh - 1].start()
    edges = ((rows - 1, top_vm, 1, hh < n_h - 1), (0, bot_vm, n_h - 1, hh > 0))

    def halo(e, f):
        row, ref, up, _ = edges[e]
        return pltpu.make_async_remote_copy(
            src_ref=x_vm.at[f, row],
            dst_ref=ref.at[f],
            send_sem=h_send.at[e],
            recv_sem=h_recv.at[e, f],
            device_id={"height": lax.rem(hh + up, n_h)},
            device_id_type=MESH,
        )

    for e in range(2):

        @pl.when(edges[e][3])
        def _():
            for f in (1, 0):
                halo(e, f).start()

    step = 64
    for c in range(3):
        with jax.named_scope("w_wait"):
            w_copies[c].wait()

        with jax.named_scope("w_trans"):
            for b in range(3):

                @pl.loop(0, channels // step)
                def _(i):
                    part = pl.ds(pl.multiple_of(i * step, step), step)
                    g0, g1, g2 = (w_vm[a, c, b, part].astype(F32) for a in range(3))
                    even = 0.5 * (g0 + g2)
                    odd = 0.5 * g1
                    u_vm[0, c, b, part] = (even + odd).astype(BF16)
                    u_vm[1, c, b, part] = (even - odd).astype(BF16)
                    u_vm[2, c, b, part] = (g1 + g2).astype(BF16)

    pltpu.make_async_copy(small, small, p_sem).wait()
    with jax.named_scope("e_shares"):
        pltpu.make_async_copy(stats.at[1:], stats.at[1:], s_recv).wait()
    total = jnp.sum(stats[...], axis=0)
    cells = n_tm * n_h * frames * rows * cols * per_group
    means = group_sums(jnp.where(own_lanes(parts), total, 0.0), parts) * (1.0 / cells)
    mean = means[:blocks]
    var = jnp.maximum(means[blocks:] - mean * mean, 0.0)
    inverse = lax.rsqrt(var + EPSILON)

    def one_row(v):
        return jnp.concatenate([v[k : k + 1] for k in range(blocks)], axis=1)

    half_scale = 0.5 * small[:, ends[0] : ends[1]] * one_row(inverse)
    half_offset = 0.5 * small[:, ends[1] : ends[2]] - one_row(mean) * half_scale

    def activate(v):
        h = v.astype(F32) * half_scale + half_offset
        return (h + h * jnp.tanh(h)).astype(BF16)

    is_first = jnp.where(tm == 0, 1, 0)
    first = is_first.astype(F32)
    F_0, F_1, LESS, PLUS, LESS_TWICE = range(5)
    at_0, at_1, at_minus = 2 * is_first, 3 - 3 * is_first, 2 + 2 * is_first

    def place_first(row, f0):
        f1 = lhs[F_1, row + 1]
        for u, value in ((F_0, f0), (LESS, f0 - f1), (PLUS, f0 + f1)):
            lhs[u, row + 1] = value

    with jax.named_scope("f_act"):
        for r in range(rows):
            lhs[F_1, r + 1] = activate(x_vm[1, r])
        for r in range(rows):
            place_first(r, activate(x_vm[0, r]))

    def edge(e, f):
        @pl.when(edges[1 - e][3])
        def _():
            halo(e, f).wait_recv()

        value = activate(edges[e][1][f])
        return jnp.where(edges[1 - e][3], value, jnp.zeros_like(value))

    m = 2 * cols
    position = lax.rem(lax.broadcasted_iota(jnp.int32, (m, 1), 0), cols)
    not_first = position != 0
    not_last = position != cols - 1
    row_sets = (tuple(range(1, rows - 1)), (0, rows - 1))

    cut = 3 * channels // 2

    def low_of(v):
        return jnp.where(not_first, pltpu.roll(v, 1, 0), 0.0)

    def high_of(v):
        return jnp.where(not_last, pltpu.roll(v, m - 1, 0), 0.0)

    def taps(u, weights, s, split=False):
        def tap(c, depth=slice(None)):
            rows_of = [
                jnp.concatenate([lhs[u, i + b] for i in row_sets[s]], axis=0) for b in range(3)
            ]
            return jnp.dot(
                jnp.concatenate(rows_of, axis=1)[:, depth],
                weights[c].reshape(3 * channels, c_out)[depth],
                preferred_element_type=F32,
            )

        halves = (slice(0, cut), slice(cut, None)) if split else (slice(None),)
        return tap(1), tap(2), *(tap(0, depth) for depth in halves)

    def merge(parts_of):
        mid, high, *low = parts_of
        value = mid + high_of(high)
        for v in low:
            value = value + low_of(v)
        return value

    def sends(s, k):
        return pltpu.make_async_remote_copy(
            src_ref=nbuf.at[s, k],
            dst_ref=rbuf.at[s, k],
            send_sem=n_send,
            recv_sem=n_recv.at[s],
            device_id={"tm": lax.rem(tm + 1, n_tm)},
            device_id_type=MESH,
        )

    def send(s, k):
        @pl.when(tm < n_tm - 1)
        def _():
            sends(s, k).start()

    bias = small[:, ends[2] : ends[3]]

    def finish(s, k, value):
        value = value + bias
        own[s, k] = value
        put(s, k, value)

    def put(s, k, value):
        value = value.astype(BF16)
        for q, i in enumerate(row_sets[s]):
            out_ref[k, i] = value[q * cols : (q + 1) * cols]

    w_0, w_1, w_2 = (w_vm.at[a] for a in range(3))
    w_half, w_half_minus, w_sum = (u_vm.at[u] for u in range(3))

    with jax.named_scope("g_inf0"):
        p_inf = merge(taps(F_1, w_0, 0, split=False))
        prod[0] = p_inf
        nbuf[0, 1] = p_inf.astype(BF16)
        ahead = taps(at_0, w_2, 0)
        send(0, 1)
        prod[1] = merge(ahead)

    with jax.named_scope("h_halo1"):
        for e, row in ((0, -1), (1, rows)):
            lhs[F_1, row + 1] = edge(e, 1)

    with jax.named_scope("i_inf1"):
        nbuf[1, 1] = merge(taps(F_1, w_0, 1, split=False)).astype(BF16)
        for r in range(rows):
            lhs[LESS_TWICE, r + 1] = lhs[LESS, r + 1] - lhs[F_1, r + 1]
        ahead = taps(at_1, w_half, 0)
        send(1, 1)
        prod[2] = merge(ahead)

    with jax.named_scope("i_rest0"):
        prod[3] = merge(taps(at_minus, w_half_minus, 0))
        p_inf, p_0, p_1, p_minus = (prod[i] for i in range(4))
        nbuf[0, 0] = (p_1 + p_minus - p_0 + first * p_inf).astype(BF16)
        finish(0, 0, jnp.where(tm == 0, 2.0 * p_1, p_0))
        finish(0, 1, jnp.where(tm == 0, 2.0 * p_1 - p_0, p_1 - p_minus - p_inf))
        ahead = taps(F_1, w_1, 1)
        send(0, 0)
        prod[1] = merge(ahead)

    with jax.named_scope("h_halo0"):
        for e, row in ((0, -1), (1, rows)):
            place_first(row, edge(e, 0))

    with jax.named_scope("j_later1"):
        prod[0] = merge(taps(F_0, w_0, 1, split=False))
        nbuf[1, 0] = (prod[0] + prod[1]).astype(BF16)
        ahead = taps(at_0, w_2, 1)
        send(1, 0)
        prod[2] = merge(ahead)

    with jax.named_scope("j_rest1"):
        prod[3] = merge(taps(at_1, w_sum, 1, split=True))
        q_2, q_3, q_4, q_5 = (prod[i] for i in range(4))
        finish(1, 0, jnp.where(tm == 0, q_2 + q_5, q_4))
        finish(1, 1, q_5 - q_4 + jnp.where(tm == 0, q_2, -q_3))

    with jax.named_scope("k_out"):
        @pl.when(tm > 0)
        def _():
            for s in range(2):
                pltpu.make_async_copy(rbuf.at[s], rbuf.at[s], n_recv.at[s]).wait()
                for k in range(2):
                    put(s, k, own[s, k] + rbuf[s, k].astype(F32))

    with jax.named_scope("l_tail"):
        pltpu.make_async_copy(stats.at[1:], stats.at[1:], s_send).wait()

        for e in range(2):

            @pl.when(edges[e][3])
            def _():
                pltpu.make_async_copy(edges[e][1], edges[e][1], h_send.at[e]).wait()

        @pl.when(tm < n_tm - 1)
        def _():
            pltpu.make_async_copy(nbuf, nbuf, n_send).wait()


def solution(mesh):
    n_tm, n_h = mesh.shape["tm"], mesh.shape["height"]

    def on_device(features, gain, shift, kernel, bias):
        frames, rows, cols, channels = features.shape
        c_out = kernel.shape[-1]
        assert frames == 2 and rows == 4
        per_set = 2 * cols
        vmem = pl.BlockSpec(memory_space=pltpu.VMEM)
        hbm = pl.BlockSpec(memory_space=pltpu.HBM)
        dma = pltpu.SemaphoreType.DMA
        return pl.pallas_call(
            functools.partial(body, n_tm, n_h),
            out_shape=pltpu.VMEM((frames, rows, cols, c_out), BF16),
            in_specs=[hbm] * 5,
            out_specs=vmem,
            scratch_shapes=[
                pltpu.VMEM((frames, rows, cols, channels), BF16),
                pltpu.VMEM((1, 2 * channels + c_out), F32),
                pltpu.VMEM((3, 3, 3, channels, c_out), BF16),
                pltpu.VMEM((3, 3, 3, channels, c_out), BF16),
                pltpu.VMEM((frames, cols, channels), BF16),
                pltpu.VMEM((frames, cols, channels), BF16),
                pltpu.VMEM((n_tm * n_h, 1, LANES), F32),
                pltpu.VMEM((5, rows + 2, cols, channels), BF16),
                pltpu.VMEM((4, per_set, c_out), F32),
                pltpu.VMEM((2, 2, per_set, c_out), F32),
                pltpu.VMEM((2, 2, per_set, c_out), BF16),
                pltpu.VMEM((2, 2, per_set, c_out), BF16),
                dma((frames, 2)),
                dma,
                dma((3,)),
                dma,
                dma,
                dma((2,)),
                dma((2, frames)),
                dma,
                dma((2,)),
            ],
            compiler_params=pltpu.CompilerParams(
                collective_id=0, has_side_effects=True, vmem_limit_bytes=67_043_328 - 640 * 2**10
            ),
        )(features, gain.reshape(1, -1), shift.reshape(1, -1), kernel, bias.reshape(1, -1))

    placed = (P(("clips", "tm"), "height", None, None), P(), P(), P(), P())
    return jax.shard_map(
        on_device,
        mesh=mesh,
        in_specs=placed,
        out_specs=P(("clips", "tm"), "height", None, None),
        check_vma=False,
    )
```

```python
import functools

import jax
import jax.numpy as jnp
from jax import lax
from jax.experimental import pallas as pl
from jax.experimental.pallas import tpu as pltpu
from jax.sharding import PartitionSpec as P

GROUPS = 32
EPSILON = 1e-06
MESH = pl.DeviceIdType.MESH
F32 = jnp.float32
BF16 = jnp.bfloat16


LANES = 128


def group_sums(values, group):
    lane = lax.rem(lax.broadcasted_iota(jnp.int32, values.shape, 1), group)
    terms = [values]
    for j in range(1, group):
        up = pltpu.roll(values, LANES - j, 1)
        down = pltpu.roll(values, group - j, 1)
        terms.append(jnp.where(lane < group - j, up, down))
    while len(terms) > 1:
        terms = [sum(terms[i : i + 2][1:], terms[i]) for i in range(0, len(terms), 2)]
    return terms[0]


def own_lanes(parts):
    lane = lax.broadcasted_iota(jnp.int32, (parts, LANES), 1)
    row = lax.broadcasted_iota(jnp.int32, (parts, LANES), 0)
    return lax.rem(lane, parts) == row


def body(
    n_tm,
    n_h,
    x_hbm,
    gain_hbm,
    shift_hbm,
    w_hbm,
    bias_hbm,
    out_ref,
    x_vm,
    x_wide,
    small,
    w_vm,
    u_vm,
    top_vm,
    bot_vm,
    stats,
    lhs,
    prod,
    own,
    nbuf,
    rbuf,
    x_sem,
    s_send,
    s_recv,
    h_send,
    h_recv,
    n_recv,
):
    frames, rows, cols, channels = x_vm.shape
    c_out = w_vm.shape[-1]
    per_group = channels // GROUPS
    tm = lax.axis_index("tm")
    hh = lax.axis_index("height")

    barrier = pltpu.get_barrier_semaphore()
    count = n_tm * n_h
    me = tm * n_h + hh

    def peer(d):
        other = lax.rem(me + d, count)
        return {"tm": lax.div(other, n_h), "height": lax.rem(other, n_h)}

    half = rows // 2
    x_copies = [
        pltpu.make_async_copy(
            x_hbm.at[f, q * half : (q + 1) * half], x_vm.at[f, q * half : (q + 1) * half], x_sem.at[f, q]
        )
        for f in range(frames)
        for q in range(2)
    ]
    for copy in x_copies:
        copy.start()
    for d in range(1, count):
        pl.semaphore_signal(barrier, inc=1, device_id=peer(d), device_id_type=MESH)
    ends = (0, channels, 2 * channels, 2 * channels + c_out)
    w_sems = (x_sem.at[0, 0], x_sem.at[0, 1], x_sem.at[1, 0])
    p_sem = x_sem.at[1, 1]
    w_copies = [
        pltpu.make_async_copy(w_hbm.at[:, :, c], w_vm.at[:, c], w_sems[c]) for c in range(3)
    ]
    with jax.named_scope("a_sums"):
        sums = jnp.zeros((8, channels), F32)
        squares = jnp.zeros((8, channels), F32)
        for p in range(2 * frames):
            with jax.named_scope("x_wait"):
                x_copies[p].wait()
            if p == 2 * frames - 1:
                for copy in w_copies:
                    copy.start()
                for i, ref in enumerate((gain_hbm, shift_hbm, bias_hbm)):
                    pltpu.make_async_copy(ref, small.at[:, ends[i] : ends[i + 1]], p_sem).start()
            f = p // 2
            for r in range(p % 2 * half, p % 2 * half + half):
                x_wide[f, r] = x_vm[f, r].astype(F32)
                v = x_wide[f, r].reshape(cols // 8, 8, channels)
                sums = sums + jnp.sum(v, axis=0)
                squares = squares + jnp.sum(v * v, axis=0)
    with jax.named_scope("b_stat"):
        blocks = channels // LANES
        parts = 2 * blocks
        assert parts <= per_group <= LANES
        sums = jnp.sum(sums, axis=0, keepdims=True)
        squares = jnp.sum(squares, axis=0, keepdims=True)
        stacked = jnp.concatenate(
            [v[:, k * LANES : (k + 1) * LANES] for v in (sums, squares) for k in range(blocks)], axis=0
        )
        spread = jnp.where(own_lanes(parts), group_sums(stacked, per_group), 0.0)
        stats[0] = jnp.sum(spread, axis=0, keepdims=True)

    with jax.named_scope("c_barrier"):
        pl.semaphore_wait(barrier, count - 1)

    shares = [
        pltpu.make_async_remote_copy(
            src_ref=stats.at[0],
            dst_ref=stats.at[d],
            send_sem=s_send,
            recv_sem=s_recv,
            device_id=peer(d),
            device_id_type=MESH,
        )
        for d in range(1, count)
    ]
    for dh in (*range(1, n_h), 0):
        for dt in range(n_tm):
            if (dt, dh) != (0, 0):
                shares[dt * n_h + dh - 1].start()
    edges = ((rows - 1, top_vm, 1, hh < n_h - 1), (0, bot_vm, n_h - 1, hh > 0))

    def halo(e, f):
        row, ref, up, _ = edges[e]
        return pltpu.make_async_remote_copy(
            src_ref=x_vm.at[f, row],
            dst_ref=ref.at[f],
            send_sem=h_send.at[e],
            recv_sem=h_recv.at[e, f],
            device_id={"height": lax.rem(hh + up, n_h)},
            device_id_type=MESH,
        )

    for e in range(2):

        @pl.when(edges[e][3])
        def _():
            for f in (1, 0):
                halo(e, f).start()

    step = 64
    for c in range(3):
        with jax.named_scope("w_wait"):
            w_copies[c].wait()

        with jax.named_scope("w_trans"):
            for b in range(3):

                @pl.loop(0, channels // step)
                def _(i):
                    part = pl.ds(pl.multiple_of(i * step, step), step)
                    g0, g1, g2 = (w_vm[a, c, b, part].astype(F32) for a in range(3))
                    even = 0.5 * (g0 + g2)
                    odd = 0.5 * g1
                    u_vm[0, c, b, part] = (even + odd).astype(BF16)
                    u_vm[1, c, b, part] = (even - odd).astype(BF16)
                    u_vm[2, c, b, part] = (g1 + g2).astype(BF16)

    pltpu.make_async_copy(small, small, p_sem).wait()
    with jax.named_scope("e_shares"):
        pltpu.make_async_copy(stats.at[1:], stats.at[1:], s_recv).wait()
        pltpu.make_async_copy(stats.at[1:], stats.at[1:], s_send).wait()
    total = jnp.sum(stats[...], axis=0)
    cells = n_tm * n_h * frames * rows * cols * per_group
    means = group_sums(jnp.where(own_lanes(parts), total, 0.0), parts) * (1.0 / cells)
    mean = means[:blocks]
    var = jnp.maximum(means[blocks:] - mean * mean, 0.0)
    inverse = lax.rsqrt(var + EPSILON)

    def one_row(v):
        return jnp.concatenate([v[k : k + 1] for k in range(blocks)], axis=1)

    half_scale = 0.5 * small[:, ends[0] : ends[1]] * one_row(inverse)
    half_offset = 0.5 * small[:, ends[1] : ends[2]] - one_row(mean) * half_scale

    def activate(v):
        h = v.astype(F32) * half_scale + half_offset
        return (h + h * jnp.tanh(h)).astype(BF16)

    is_first = jnp.where(tm == 0, 1, 0)
    first = is_first.astype(F32)
    F_0, F_1, LESS, PLUS, LESS_TWICE = range(5)
    at_0, at_1, at_minus = 2 * is_first, 3 - 3 * is_first, 2 + 2 * is_first

    def place_first(row, f0):
        f1 = lhs[F_1, row + 1]
        for u, value in ((F_0, f0), (LESS, f0 - f1), (PLUS, f0 + f1)):
            lhs[u, row + 1] = value

    with jax.named_scope("f_act"):
        for r in range(rows):
            lhs[F_1, r + 1] = activate(x_wide[1, r])
        for r in range(rows):
            place_first(r, activate(x_wide[0, r]))

    def arrived(e, f):
        @pl.when(edges[1 - e][3])
        def _():
            halo(e, f).wait_recv()

    def edge(e, f):
        value = activate(edges[e][1][f])
        return jnp.where(edges[1 - e][3], value, jnp.zeros_like(value))

    m = 2 * cols
    position = lax.rem(lax.broadcasted_iota(jnp.int32, (m, 1), 0), cols)
    not_first = position != 0
    not_last = position != cols - 1
    row_sets = (tuple(range(1, rows - 1)), (0, rows - 1))

    cut = 3 * channels // 2

    def low_of(v):
        return jnp.where(not_first, pltpu.roll(v, 1, 0), 0.0)

    def high_of(v):
        return jnp.where(not_last, pltpu.roll(v, m - 1, 0), 0.0)

    def tap(u, weights, s, c, depth=slice(None)):
        rows_of = [jnp.concatenate([lhs[u, i + b] for i in row_sets[s]], axis=0) for b in range(3)]
        return jnp.dot(
            jnp.concatenate(rows_of, axis=1)[:, depth],
            weights[c].reshape(3 * channels, c_out)[depth],
            preferred_element_type=F32,
        )

    def lows(u, weights, s, split=True):
        halves = (slice(0, cut), slice(cut, None)) if split else (slice(None),)
        return [tap(u, weights, s, 0, depth) for depth in halves]

    def taps(u, weights, s, split=False):
        high, low = tap(u, weights, s, 2), lows(u, weights, s, split)
        return tap(u, weights, s, 1), high, *low

    def merge(parts_of):
        mid, high, *low = parts_of
        value = high_of(high)
        for v in low:
            value = value + low_of(v)
        return value + mid

    def sends(s, k):
        return pltpu.make_async_remote_copy(
            src_ref=nbuf.at[s, k],
            dst_ref=rbuf.at[s, k],
            send_sem=s_send,
            recv_sem=n_recv.at[s],
            device_id={"tm": lax.rem(tm + 1, n_tm)},
            device_id_type=MESH,
        )

    def send(s, k):
        @pl.when(tm < n_tm - 1)
        def _():
            sends(s, k).start()

    bias = small[:, ends[2] : ends[3]]

    def finish(s, k, value):
        value = value + bias
        own[s, k] = value
        put(s, k, value)

    def put(s, k, value):
        value = value.astype(BF16)
        for q, i in enumerate(row_sets[s]):
            out_ref[k, i] = value[q * cols : (q + 1) * cols]

    w_0, w_1, w_2 = (w_vm.at[a] for a in range(3))
    w_half, w_half_minus, w_sum = (u_vm.at[u] for u in range(3))

    with jax.named_scope("g_inf0"):
        p_inf = merge(taps(F_1, w_0, 0))
        prod[0] = p_inf
        nbuf[0, 1] = p_inf.astype(BF16)
        ahead = taps(at_0, w_2, 0)
        send(0, 1)
        prod[1] = merge(ahead)
        beside = tap(at_1, w_half, 0, 2)
        prod[2] = high_of(beside)

    with jax.named_scope("h_halo1"):
        for e in range(2):
            arrived(e, 1)

    with jax.named_scope("i_inf1"):
        mid = tap(at_1, w_half, 0, 1)
        for e, row in ((0, -1), (1, rows)):
            lhs[F_1, row + 1] = edge(e, 1)
        prod[2] = prod[2] + mid
        nbuf[1, 1] = merge(taps(F_1, w_0, 1)).astype(BF16)
        for r in range(rows):
            lhs[LESS_TWICE, r + 1] = lhs[LESS, r + 1] - lhs[F_1, r + 1]
        send(1, 1)
        (low,) = lows(at_1, w_half, 0, False)
        high = tap(at_minus, w_half_minus, 0, 2)
        prod[2] = prod[2] + low_of(low)

    with jax.named_scope("i_rest0"):
        (low,) = lows(at_minus, w_half_minus, 0, False)
        prod[3] = merge((tap(at_minus, w_half_minus, 0, 1), high, low))
        p_inf, p_0, p_1, p_minus = (prod[i] for i in range(4))
        nbuf[0, 0] = (p_1 + p_minus - p_0 + first * p_inf).astype(BF16)
        finish(0, 0, jnp.where(tm == 0, 2.0 * p_1, p_0))
        finish(0, 1, jnp.where(tm == 0, 2.0 * p_1 - p_0, p_1 - p_minus - p_inf))
        ahead = (tap(F_1, w_1, 1, 2), *lows(F_1, w_1, 1, False))
        send(0, 0)
        prod[1] = high_of(ahead[0]) + low_of(ahead[1])

    with jax.named_scope("h_halo0"):
        for e in range(2):
            arrived(e, 0)

    with jax.named_scope("j_later1"):
        mid = tap(F_1, w_1, 1, 1)
        for e, row in ((0, -1), (1, rows)):
            place_first(row, edge(e, 0))
        prod[1] = prod[1] + mid
        prod[0] = merge(taps(F_0, w_0, 1))
        nbuf[1, 0] = (prod[0] + prod[1]).astype(BF16)
        ahead = taps(at_0, w_2, 1)
        send(1, 0)
        prod[2] = merge(ahead)

    with jax.named_scope("j_rest1"):
        prod[3] = merge(taps(at_1, w_sum, 1))
        q_2, q_3, q_4, q_5 = (prod[i] for i in range(4))
        finish(1, 0, jnp.where(tm == 0, q_2 + q_5, q_4))
        finish(1, 1, q_5 - q_4 + jnp.where(tm == 0, q_2, -q_3))

    with jax.named_scope("k_out"):
        @pl.when(tm > 0)
        def _():
            for s in range(2):
                pltpu.make_async_copy(rbuf.at[s], rbuf.at[s], n_recv.at[s]).wait()
                for k in range(2):
                    put(s, k, own[s, k] + rbuf[s, k].astype(F32))

    with jax.named_scope("l_tail"):
        for e in range(2):

            @pl.when(edges[e][3])
            def _():
                pltpu.make_async_copy(edges[e][1], edges[e][1], h_send.at[e]).wait()

        @pl.when(tm < n_tm - 1)
        def _():
            pltpu.make_async_copy(nbuf, nbuf, s_send).wait()


def solution(mesh):
    n_tm, n_h = mesh.shape["tm"], mesh.shape["height"]

    def on_device(features, gain, shift, kernel, bias):
        frames, rows, cols, channels = features.shape
        c_out = kernel.shape[-1]
        assert frames == 2 and rows == 4
        per_set = 2 * cols
        vmem = pl.BlockSpec(memory_space=pltpu.VMEM)
        hbm = pl.BlockSpec(memory_space=pltpu.HBM)
        dma = pltpu.SemaphoreType.DMA
        return pl.pallas_call(
            functools.partial(body, n_tm, n_h),
            out_shape=pltpu.VMEM((frames, rows, cols, c_out), BF16),
            in_specs=[hbm] * 5,
            out_specs=vmem,
            scratch_shapes=[
                pltpu.VMEM((frames, rows, cols, channels), BF16),
                pltpu.VMEM((frames, rows, cols, channels), F32),
                pltpu.VMEM((1, 2 * channels + c_out), F32),
                pltpu.VMEM((3, 3, 3, channels, c_out), BF16),
                pltpu.VMEM((3, 3, 3, channels, c_out), BF16),
                pltpu.VMEM((frames, cols, channels), BF16),
                pltpu.VMEM((frames, cols, channels), BF16),
                pltpu.VMEM((n_tm * n_h, 1, LANES), F32),
                pltpu.VMEM((5, rows + 2, cols, channels), BF16),
                pltpu.VMEM((4, per_set, c_out), F32),
                pltpu.VMEM((2, 2, per_set, c_out), F32),
                pltpu.VMEM((2, 2, per_set, c_out), BF16),
                pltpu.VMEM((2, 2, per_set, c_out), BF16),
                dma((frames, 2)),
                dma,
                dma,
                dma((2,)),
                dma((2, frames)),
                dma((2,)),
            ],
            compiler_params=pltpu.CompilerParams(
                collective_id=0, has_side_effects=True, vmem_limit_bytes=67_043_328 - 640 * 2**10
            ),
        )(features, gain.reshape(1, -1), shift.reshape(1, -1), kernel, bias.reshape(1, -1))

    placed = (P(("clips", "tm"), "height", None, None), P(), P(), P(), P())
    return jax.shard_map(
        on_device,
        mesh=mesh,
        in_specs=placed,
        out_specs=P(("clips", "tm"), "height", None, None),
        check_vma=False,
    )
```

```python
import functools

import jax
import jax.numpy as jnp
from jax import lax
from jax.experimental import pallas as pl
from jax.experimental.pallas import tpu as pltpu
from jax.sharding import PartitionSpec as P

GROUPS = 32
EPSILON = 1e-06
MESH = pl.DeviceIdType.MESH
F32 = jnp.float32
BF16 = jnp.bfloat16


LANES = 128


def group_sums(values, group):
    lane = lax.rem(lax.broadcasted_iota(jnp.int32, values.shape, 1), group)
    terms = [values]
    for j in range(1, group):
        up = pltpu.roll(values, LANES - j, 1)
        down = pltpu.roll(values, group - j, 1)
        terms.append(jnp.where(lane < group - j, up, down))
    while len(terms) > 1:
        terms = [sum(terms[i : i + 2][1:], terms[i]) for i in range(0, len(terms), 2)]
    return terms[0]


def own_lanes(parts):
    lane = lax.broadcasted_iota(jnp.int32, (parts, LANES), 1)
    row = lax.broadcasted_iota(jnp.int32, (parts, LANES), 0)
    return lax.rem(lane, parts) == row


def body(
    n_tm,
    n_h,
    x_hbm,
    gain_hbm,
    shift_hbm,
    w_hbm,
    bias_hbm,
    out_ref,
    x_vm,
    x_wide,
    small,
    w_vm,
    u_vm,
    top_vm,
    bot_vm,
    stats,
    lhs,
    prod,
    own,
    nbuf,
    rbuf,
    x_sem,
    s_send,
    s_recv,
    h_send,
    h_recv,
    n_recv,
):
    frames, rows, cols, channels = x_vm.shape
    c_out = w_vm.shape[-1]
    per_group = channels // GROUPS
    tm = lax.axis_index("tm")
    hh = lax.axis_index("height")

    barrier = pltpu.get_barrier_semaphore()
    count = n_tm * n_h
    me = tm * n_h + hh

    def peer(d):
        other = lax.rem(me + d, count)
        return {"tm": lax.div(other, n_h), "height": lax.rem(other, n_h)}

    half = rows // 2
    x_copies = [
        pltpu.make_async_copy(
            x_hbm.at[f, q * half : (q + 1) * half], x_vm.at[f, q * half : (q + 1) * half], x_sem.at[f, q]
        )
        for f in range(frames)
        for q in range(2)
    ]
    for copy in x_copies:
        copy.start()
    for d in range(1, count):
        pl.semaphore_signal(barrier, inc=1, device_id=peer(d), device_id_type=MESH)
    ends = (0, channels, 2 * channels, 2 * channels + c_out)
    w_sems = (x_sem.at[0, 0], x_sem.at[0, 1], x_sem.at[1, 0])
    p_sem = x_sem.at[1, 1]
    w_copies = [
        pltpu.make_async_copy(w_hbm.at[:, :, c], w_vm.at[:, c], w_sems[c]) for c in range(3)
    ]
    with jax.named_scope("a_sums"):
        sums = jnp.zeros((8, channels), F32)
        squares = jnp.zeros((8, channels), F32)
        for p in range(2 * frames):
            with jax.named_scope("x_wait"):
                x_copies[p].wait()
            if p == 2 * frames - 1:
                for copy in w_copies:
                    copy.start()
                for i, ref in enumerate((gain_hbm, shift_hbm, bias_hbm)):
                    pltpu.make_async_copy(ref, small.at[:, ends[i] : ends[i + 1]], p_sem).start()
            f = p // 2
            for r in range(p % 2 * half, p % 2 * half + half):
                x_wide[f, r] = x_vm[f, r].astype(F32)
                v = x_wide[f, r].reshape(cols // 8, 8, channels)
                sums = sums + jnp.sum(v, axis=0)
                squares = squares + jnp.sum(v * v, axis=0)
    with jax.named_scope("b_stat"):
        blocks = channels // LANES
        parts = 2 * blocks
        assert parts <= per_group <= LANES
        sums = jnp.sum(sums, axis=0, keepdims=True)
        squares = jnp.sum(squares, axis=0, keepdims=True)
        stacked = jnp.concatenate(
            [v[:, k * LANES : (k + 1) * LANES] for v in (sums, squares) for k in range(blocks)], axis=0
        )
        spread = jnp.where(own_lanes(parts), group_sums(stacked, per_group), 0.0)
        stats[0] = jnp.sum(spread, axis=0, keepdims=True)

    with jax.named_scope("c_barrier"):
        pl.semaphore_wait(barrier, count - 1)

    shares = [
        pltpu.make_async_remote_copy(
            src_ref=stats.at[0],
            dst_ref=stats.at[d],
            send_sem=s_send,
            recv_sem=s_recv,
            device_id=peer(d),
            device_id_type=MESH,
        )
        for d in range(1, count)
    ]
    for dh in (*range(1, n_h), 0):
        for dt in range(n_tm):
            if (dt, dh) != (0, 0):
                shares[dt * n_h + dh - 1].start()
    edges = ((rows - 1, top_vm, 1, hh < n_h - 1), (0, bot_vm, n_h - 1, hh > 0))

    def halo(e, f):
        row, ref, up, _ = edges[e]
        return pltpu.make_async_remote_copy(
            src_ref=x_vm.at[f, row],
            dst_ref=ref.at[f],
            send_sem=h_send.at[e],
            recv_sem=h_recv.at[e, f],
            device_id={"height": lax.rem(hh + up, n_h)},
            device_id_type=MESH,
        )

    for e in range(2):

        @pl.when(edges[e][3])
        def _():
            for f in (1, 0):
                halo(e, f).start()

    step = 64
    for c in range(3):
        with jax.named_scope("w_wait"):
            w_copies[c].wait()

        with jax.named_scope("w_trans"):
            for b in range(3):

                @pl.loop(0, channels // step)
                def _(i):
                    part = pl.ds(pl.multiple_of(i * step, step), step)
                    g0, g1, g2 = (w_vm[a, c, b, part].astype(F32) for a in range(3))
                    even = 0.5 * (g0 + g2)
                    odd = 0.5 * g1
                    u_vm[0, c, b, part] = (even + odd).astype(BF16)
                    u_vm[1, c, b, part] = (even - odd).astype(BF16)
                    u_vm[2, c, b, part] = (g1 + g2).astype(BF16)

    pltpu.make_async_copy(small, small, p_sem).wait()
    with jax.named_scope("e_shares"):
        pltpu.make_async_copy(stats.at[1:], stats.at[1:], s_recv).wait()
        pltpu.make_async_copy(stats.at[1:], stats.at[1:], s_send).wait()
    total = jnp.sum(stats[...], axis=0)
    cells = n_tm * n_h * frames * rows * cols * per_group
    means = group_sums(jnp.where(own_lanes(parts), total, 0.0), parts) * (1.0 / cells)
    mean = means[:blocks]
    var = jnp.maximum(means[blocks:] - mean * mean, 0.0)
    inverse = lax.rsqrt(var + EPSILON)

    def one_row(v):
        return jnp.concatenate([v[k : k + 1] for k in range(blocks)], axis=1)

    half_scale = 0.5 * small[:, ends[0] : ends[1]] * one_row(inverse)
    half_offset = 0.5 * small[:, ends[1] : ends[2]] - one_row(mean) * half_scale

    def activate(v):
        h = v.astype(F32) * half_scale + half_offset
        return (h + h * jnp.tanh(h)).astype(BF16)

    is_first = jnp.where(tm == 0, 1, 0)
    first = is_first.astype(F32)
    F_0, F_1, LESS, PLUS, LESS_TWICE = range(5)
    at_0, at_1, at_minus = 2 * is_first, 3 - 3 * is_first, 2 + 2 * is_first

    def place_first(row, f0):
        f1 = lhs[F_1, row + 1]
        for u, value in ((F_0, f0), (LESS, f0 - f1), (PLUS, f0 + f1)):
            lhs[u, row + 1] = value

    with jax.named_scope("f_act"):
        for r in range(rows):
            lhs[F_1, r + 1] = activate(x_wide[1, r])
        for r in range(rows):
            place_first(r, activate(x_wide[0, r]))

    def arrived(e, f):
        @pl.when(edges[1 - e][3])
        def _():
            halo(e, f).wait_recv()

    def edge(e, f):
        value = activate(edges[e][1][f])
        return jnp.where(edges[1 - e][3], value, jnp.zeros_like(value))

    m = 2 * cols
    position = lax.rem(lax.broadcasted_iota(jnp.int32, (m, 1), 0), cols)
    not_first = position != 0
    not_last = position != cols - 1
    row_sets = (tuple(range(1, rows - 1)), (0, rows - 1))

    cut = 3 * channels // 2

    def low_of(v):
        return jnp.where(not_first, pltpu.roll(v, 1, 0), 0.0)

    def high_of(v):
        return jnp.where(not_last, pltpu.roll(v, m - 1, 0), 0.0)

    def tap(u, weights, s, c, depth=slice(None)):
        rows_of = [jnp.concatenate([lhs[u, i + b] for i in row_sets[s]], axis=0) for b in range(3)]
        return jnp.dot(
            jnp.concatenate(rows_of, axis=1)[:, depth],
            weights[c].reshape(3 * channels, c_out)[depth],
            preferred_element_type=F32,
        )

    def lows(u, weights, s, split=True):
        halves = (slice(0, cut), slice(cut, None)) if split else (slice(None),)
        return [tap(u, weights, s, 0, depth) for depth in halves]

    def taps(u, weights, s, split=False):
        high, low = tap(u, weights, s, 2), lows(u, weights, s, split)
        return tap(u, weights, s, 1), high, *low

    def merge(parts_of):
        mid, high, *low = parts_of
        value = high_of(high)
        for v in low:
            value = value + low_of(v)
        return value + mid

    def sends(s, k):
        return pltpu.make_async_remote_copy(
            src_ref=nbuf.at[s, k],
            dst_ref=rbuf.at[s, k],
            send_sem=s_send,
            recv_sem=n_recv.at[s],
            device_id={"tm": lax.rem(tm + 1, n_tm)},
            device_id_type=MESH,
        )

    def send(s, k):
        @pl.when(tm < n_tm - 1)
        def _():
            sends(s, k).start()

    bias = small[:, ends[2] : ends[3]]

    def finish(s, k, value):
        value = value + bias
        own[s, k] = value
        put(s, k, value)

    def put(s, k, value):
        value = value.astype(BF16)
        for q, i in enumerate(row_sets[s]):
            out_ref[k, i] = value[q * cols : (q + 1) * cols]

    w_0, w_1, w_2 = (w_vm.at[a] for a in range(3))
    w_half, w_half_minus, w_sum = (u_vm.at[u] for u in range(3))

    with jax.named_scope("g_inf0"):
        p_inf = merge(taps(F_1, w_0, 0))
        prod[0] = p_inf
        nbuf[0, 1] = p_inf.astype(BF16)
        ahead = taps(at_0, w_2, 0)
        send(0, 1)
        prod[1] = merge(ahead)
        beside = tap(at_1, w_half, 0, 2)
        prod[2] = high_of(beside)

    with jax.named_scope("h_halo1"):
        for e in range(2):
            arrived(e, 1)

    with jax.named_scope("i_inf1"):
        mid = tap(at_1, w_half, 0, 1)
        for e, row in ((0, -1), (1, rows)):
            lhs[F_1, row + 1] = edge(e, 1)
        prod[2] = prod[2] + mid
        nbuf[1, 1] = merge(taps(F_1, w_0, 1)).astype(BF16)
        for r in range(rows):
            lhs[LESS_TWICE, r + 1] = lhs[LESS, r + 1] - lhs[F_1, r + 1]
        send(1, 1)
        (low,) = lows(at_1, w_half, 0, False)
        high = tap(at_minus, w_half_minus, 0, 2)
        prod[2] = prod[2] + low_of(low)

    with jax.named_scope("i_rest0"):
        (low,) = lows(at_minus, w_half_minus, 0, False)
        prod[3] = merge((tap(at_minus, w_half_minus, 0, 1), high, low))
        p_inf, p_0, p_1, p_minus = (prod[i] for i in range(4))
        nbuf[0, 0] = (p_1 + p_minus - p_0 + first * p_inf).astype(BF16)
        finish(0, 0, jnp.where(tm == 0, 2.0 * p_1, p_0))
        finish(0, 1, jnp.where(tm == 0, 2.0 * p_1 - p_0, p_1 - p_minus - p_inf))
        ahead = (tap(F_1, w_1, 1, 2), *lows(F_1, w_1, 1, False))
        send(0, 0)
        for e in range(2):
            arrived(e, 0)

    with jax.named_scope("j_later1"):
        mid = tap(F_1, w_1, 1, 1)
        for e, row in ((0, -1), (1, rows)):
            place_first(row, edge(e, 0))
        prod[1] = merge((mid, *ahead))
        prod[0] = merge(taps(F_0, w_0, 1))
        nbuf[1, 0] = (prod[0] + prod[1]).astype(BF16)
        ahead = (tap(at_0, w_2, 1, 2), *lows(at_0, w_2, 1, False))
        send(1, 0)

    with jax.named_scope("j_rest1"):
        q_2, q_3 = prod[0], prod[1]
        sides_4 = high_of(ahead[0]) + low_of(ahead[1])
        prod[2] = sides_4
        sides_5 = high_of(tap(at_1, w_sum, 1, 2)) + low_of(*lows(at_1, w_sum, 1, False))
        prod[3] = sides_5 - prod[2] + jnp.where(tm == 0, q_2, -q_3)
        prod[2] = jnp.where(tm == 0, q_2 + sides_5, prod[2])
        mid_5, mid_4 = tap(at_1, w_sum, 1, 1), tap(at_0, w_2, 1, 1)
        finish(1, 0, prod[2] + jnp.where(tm == 0, mid_5, mid_4))
        finish(1, 1, prod[3] + (mid_5 - mid_4))

    with jax.named_scope("k_out"):
        @pl.when(tm > 0)
        def _():
            for s in range(2):
                pltpu.make_async_copy(rbuf.at[s], rbuf.at[s], n_recv.at[s]).wait()
                for k in range(2):
                    put(s, k, own[s, k] + rbuf[s, k].astype(F32))

    with jax.named_scope("l_tail"):
        for e in range(2):

            @pl.when(edges[e][3])
            def _():
                pltpu.make_async_copy(edges[e][1], edges[e][1], h_send.at[e]).wait()

        @pl.when(tm < n_tm - 1)
        def _():
            pltpu.make_async_copy(nbuf, nbuf, s_send).wait()


def solution(mesh):
    n_tm, n_h = mesh.shape["tm"], mesh.shape["height"]

    def on_device(features, gain, shift, kernel, bias):
        frames, rows, cols, channels = features.shape
        c_out = kernel.shape[-1]
        assert frames == 2 and rows == 4
        per_set = 2 * cols
        vmem = pl.BlockSpec(memory_space=pltpu.VMEM)
        hbm = pl.BlockSpec(memory_space=pltpu.HBM)
        dma = pltpu.SemaphoreType.DMA
        return pl.pallas_call(
            functools.partial(body, n_tm, n_h),
            out_shape=pltpu.VMEM((frames, rows, cols, c_out), BF16),
            in_specs=[hbm] * 5,
            out_specs=vmem,
            scratch_shapes=[
                pltpu.VMEM((frames, rows, cols, channels), BF16),
                pltpu.VMEM((frames, rows, cols, channels), F32),
                pltpu.VMEM((1, 2 * channels + c_out), F32),
                pltpu.VMEM((3, 3, 3, channels, c_out), BF16),
                pltpu.VMEM((3, 3, 3, channels, c_out), BF16),
                pltpu.VMEM((frames, cols, channels), BF16),
                pltpu.VMEM((frames, cols, channels), BF16),
                pltpu.VMEM((n_tm * n_h, 1, LANES), F32),
                pltpu.VMEM((5, rows + 2, cols, channels), BF16),
                pltpu.VMEM((4, per_set, c_out), F32),
                pltpu.VMEM((2, 2, per_set, c_out), F32),
                pltpu.VMEM((2, 2, per_set, c_out), BF16),
                pltpu.VMEM((2, 2, per_set, c_out), BF16),
                dma((frames, 2)),
                dma,
                dma,
                dma((2,)),
                dma((2, frames)),
                dma((2,)),
            ],
            compiler_params=pltpu.CompilerParams(
                collective_id=0, has_side_effects=True, vmem_limit_bytes=67_043_328 - 640 * 2**10
            ),
        )(features, gain.reshape(1, -1), shift.reshape(1, -1), kernel, bias.reshape(1, -1))

    placed = (P(("clips", "tm"), "height", None, None), P(), P(), P(), P())
    return jax.shard_map(
        on_device,
        mesh=mesh,
        in_specs=placed,
        out_specs=P(("clips", "tm"), "height", None, None),
        check_vma=False,
    )
```
